16 devices in a mesh: tp: 16 (over z, y, x, core).
Axes of the slice: x: 2, y: 2, z: 2, core: 2. Of those that a mesh axis runs over, the one named last changes fastest.
Arguments:
- x_input: bfloat16 [2, 2048, 4096], P(None, 'tp')
- w_query: bfloat16 [4096, 4096], P(None, 'tp')
- w_key: bfloat16 [4096, 4096], P(None, 'tp')
- w_value: bfloat16 [4096, 4096], P(None, 'tp')
- w_out: bfloat16 [4096, 4096], P('tp')
- g_query: bfloat16 [4096], P('tp')
- g_key: bfloat16 [4096], P('tp')
- g_attn: bfloat16 [4096], replicated
- grad_y: bfloat16 [2, 2048, 4096], P(None, 'tp')
Outputs:
- output 1: bfloat16 [2, 2048, 4096], P(None, 'tp')
- output 2: bfloat16 [2, 2048, 4096], P(None, 'tp')
- output 3: bfloat16 [4096, 4096], P(None, 'tp')
- output 4: bfloat16 [4096, 4096], P(None, 'tp')
- output 5: bfloat16 [4096, 4096], P(None, 'tp')
- output 6: bfloat16 [4096, 4096], P('tp')
- output 7: bfloat16 [4096], P('tp')
- output 8: bfloat16 [4096], P('tp')
- output 9: bfloat16 [4096], replicated
All inputs are finite; a program needn't handle non-finite values.
Results may differ from the reference program's by a relative error of at most 0.0178161.
Values are sent between devices in bfloat16 or wider.
A program may use at most 1 GiB of HBM per device.

```python
import jax
import jax.numpy as jnp
from jax import lax

BATCH_SIZE = 2
SEQ_LEN = 2048
MODEL_DIM = 4096
NUM_HEADS = 32
HEAD_DIM = 128
ROPE_THETA = 500000
NORM_EPS = 1e-6


def setup_inputs(seed: int = 0) -> dict:
    rng_keys = jax.random.split(jax.random.key(seed), 12)
    fan_scale = MODEL_DIM ** -0.5
    act_shape = (BATCH_SIZE, SEQ_LEN, MODEL_DIM)
    mat_shape = (MODEL_DIM, MODEL_DIM)
    head_q = jnp.exp(jax.random.uniform(rng_keys[0], (NUM_HEADS,), jnp.float32, jnp.log(0.3), jnp.log(3.0)))
    head_k = jnp.exp(jax.random.uniform(rng_keys[1], (NUM_HEADS,), jnp.float32, jnp.log(0.3), jnp.log(3.0)))
    col_q = jnp.repeat(head_q, HEAD_DIM)[None, :]
    col_k = jnp.repeat(head_k, HEAD_DIM)[None, :]
    x_input = jax.random.normal(rng_keys[2], act_shape, jnp.float32)
    w_query = jax.random.normal(rng_keys[3], mat_shape, jnp.float32) * fan_scale * col_q
    w_key = jax.random.normal(rng_keys[4], mat_shape, jnp.float32) * fan_scale * col_k
    w_value = jax.random.normal(rng_keys[5], mat_shape, jnp.float32) * fan_scale
    w_out = jax.random.normal(rng_keys[6], mat_shape, jnp.float32) * fan_scale
    g_query = jax.random.uniform(rng_keys[7], (MODEL_DIM,), jnp.float32, 0.5, 1.5)
    g_key = jax.random.uniform(rng_keys[8], (MODEL_DIM,), jnp.float32, 0.5, 1.5)
    g_attn = jax.random.uniform(rng_keys[9], (MODEL_DIM,), jnp.float32, 0.5, 1.5)
    grad_y = jax.random.normal(rng_keys[10], act_shape, jnp.float32)
    return {'x_input': x_input.astype(jnp.bfloat16), 'w_query': w_query.astype(jnp.bfloat16), 'w_key': w_key.astype(jnp.bfloat16), 'w_value': w_value.astype(jnp.bfloat16), 'w_out': w_out.astype(jnp.bfloat16), 'g_query': g_query.astype(jnp.bfloat16), 'g_key': g_key.astype(jnp.bfloat16), 'g_attn': g_attn.astype(jnp.bfloat16), 'grad_y': grad_y.astype(jnp.bfloat16)}


def rope_tables():
    half_dim = HEAD_DIM // 2
    inv_freq = 1.0 / (ROPE_THETA ** (jnp.arange(half_dim, dtype=jnp.float32) / half_dim))
    angles = jnp.arange(SEQ_LEN, dtype=jnp.float32)[:, None] * inv_freq[None, :]
    return jnp.cos(angles)[:, None, :], jnp.sin(angles)[:, None, :]


def rotate(values, cos_t, sin_t):
    lower_half, upper_half = jnp.split(values, 2, axis=-1)
    return jnp.concatenate([lower_half * cos_t - upper_half * sin_t, upper_half * cos_t + lower_half * sin_t], axis=-1)


def whole_norm(values, gain):
    inv_rms = lax.rsqrt(jnp.mean(values * values, axis=-1, keepdims=True) + NORM_EPS)
    return values * inv_rms * gain.astype(jnp.float32)


def head_attention(operands):
    q_head, k_head, v_head = operands
    scores = jnp.einsum('bqd,bkd->bqk', q_head.astype(jnp.float32), k_head.astype(jnp.float32)) * (HEAD_DIM ** -0.5)
    causal = jnp.arange(SEQ_LEN)[:, None] >= jnp.arange(SEQ_LEN)[None, :]
    attn_probs = jax.nn.softmax(jnp.where(causal[None], scores, -1e30), axis=-1)
    head_out = jnp.einsum('bqk,bkd->bqd', attn_probs.astype(jnp.bfloat16).astype(jnp.float32), v_head.astype(jnp.float32))
    return head_out.astype(jnp.bfloat16)


def block_forward(x_input, w_query, w_key, w_value, w_out, g_query, g_key, g_attn):
    x_rows = x_input.reshape(BATCH_SIZE * SEQ_LEN, MODEL_DIM)
    head_shape = (BATCH_SIZE, SEQ_LEN, NUM_HEADS, HEAD_DIM)
    cos_t, sin_t = rope_tables()
    q_raw = jnp.dot(x_rows, w_query, preferred_element_type=jnp.float32)
    k_raw = jnp.dot(x_rows, w_key, preferred_element_type=jnp.float32)
    v_proj = jnp.dot(x_rows, w_value, preferred_element_type=jnp.float32).astype(jnp.bfloat16)
    q_rot = rotate(whole_norm(q_raw, g_query).reshape(head_shape), cos_t, sin_t).astype(jnp.bfloat16)
    k_rot = rotate(whole_norm(k_raw, g_key).reshape(head_shape), cos_t, sin_t).astype(jnp.bfloat16)
    v_heads = v_proj.reshape(head_shape)
    per_head = lax.map(jax.checkpoint(head_attention), (jnp.moveaxis(q_rot, 2, 0), jnp.moveaxis(k_rot, 2, 0), jnp.moveaxis(v_heads, 2, 0)))
    attn_rows = jnp.moveaxis(per_head, 0, 2).reshape(BATCH_SIZE * SEQ_LEN, MODEL_DIM)
    attn_sum = jnp.dot(attn_rows, w_out, preferred_element_type=jnp.float32)
    post_rms = lax.rsqrt(jnp.mean(attn_sum * attn_sum, axis=-1, keepdims=True) + NORM_EPS)
    y_rows = x_rows.astype(jnp.float32) + attn_sum * post_rms * g_attn.astype(jnp.float32)
    return y_rows.astype(jnp.bfloat16).reshape(BATCH_SIZE, SEQ_LEN, MODEL_DIM)


def reference(x_input, w_query, w_key, w_value, w_out, g_query, g_key, g_attn, grad_y):
    y_out, pullback = jax.vjp(block_forward, x_input, w_query, w_key, w_value, w_out, g_query, g_key, g_attn)
    grad_x, grad_wq, grad_wk, grad_wv, grad_wo, grad_gq, grad_gk, grad_ga = pullback(grad_y)
    return (y_out, grad_x, grad_wq, grad_wk, grad_wv, grad_wo, grad_gq, grad_gk, grad_ga)
```

```python
import functools
import math

import jax
import jax.numpy as jnp
from jax import lax
from jax.experimental import pallas as pl
from jax.experimental.pallas import tpu as pltpu
from jax.sharding import PartitionSpec as P

HEAD_SIZE = 128
ROPE_THETA = 500000.0
NORM_EPS = 1e-6
N_DEV = 16
Q_BLOCK = 256
LOG2E = math.log2(math.e)
ATTN_SCALE = HEAD_SIZE ** -0.5
NT = (((1,), (1,)), ((), ()))
NN = (((1,), (0,)), ((), ()))


def rope_tables(seq_len):
    half_dim = HEAD_SIZE // 2
    inv_freq = 1.0 / (ROPE_THETA ** (jnp.arange(half_dim, dtype=jnp.float32) / half_dim))
    angles = jnp.arange(seq_len, dtype=jnp.float32)[:, None] * inv_freq[None, :]
    cos_t, sin_t = jnp.cos(angles), jnp.sin(angles)
    return jnp.concatenate([cos_t, cos_t], axis=-1), jnp.concatenate([-sin_t, sin_t], axis=-1)


def vmem_spec():
    return pl.BlockSpec(memory_space=pltpu.VMEM)


def sum_kernel(part_ref, out_ref, slots, send_sems, recv_sems):
    me = lax.axis_index('tp')
    copies = []
    for step in range(1, N_DEV):
        peer = lax.rem(me + step, N_DEV)
        copy = pltpu.make_async_remote_copy(
            src_ref=part_ref, dst_ref=slots.at[step], send_sem=send_sems.at[step], recv_sem=recv_sems.at[step],
            device_id=(peer,), device_id_type=pl.DeviceIdType.MESH)
        copy.start()
        copies.append(copy)
    slots[0] = part_ref[...]
    for copy in copies:
        copy.wait()
    total = jnp.zeros(part_ref.shape, jnp.float32)
    for owner in range(N_DEV):
        total = total + slots[lax.rem(me - owner + N_DEV, N_DEV)]
    out_ref[...] = total


def sum_devices(part):
    return pl.pallas_call(
        sum_kernel,
        out_shape=jax.ShapeDtypeStruct(part.shape, jnp.float32),
        in_specs=[vmem_spec()],
        out_specs=vmem_spec(),
        scratch_shapes=[pltpu.VMEM((N_DEV,) + part.shape, jnp.float32),
                        pltpu.SemaphoreType.DMA((N_DEV,)), pltpu.SemaphoreType.DMA((N_DEV,))],
        compiler_params=pltpu.CompilerParams(has_side_effects=True),
        cost_estimate=pl.CostEstimate(flops=int(1e9), bytes_accessed=int(1e6), transcendentals=0),
        name='sum_devices',
    )(part)


def to_tokens_kernel(n_arr, tok, cols, *refs):
    ins, outs = refs[:n_arr], refs[n_arr:-2]
    send_sems, recv_sems = refs[-2:]
    me = lax.axis_index('tp')
    copies = []
    my_cols = pl.ds(pl.multiple_of(me * cols, cols), cols)
    for step in range(1, N_DEV):
        peer = lax.rem(me + step, N_DEV)
        rows = pl.ds(pl.multiple_of(peer * tok, tok), tok)
        for i in range(n_arr):
            copy = pltpu.make_async_remote_copy(
                src_ref=ins[i].at[rows, :], dst_ref=outs[i // 2].at[i % 2, :, my_cols],
                send_sem=send_sems.at[i, step], recv_sem=recv_sems.at[i, step],
                device_id=(peer,), device_id_type=pl.DeviceIdType.MESH)
            copy.start()
            copies.append(copy)
    my_rows = pl.ds(pl.multiple_of(me * tok, tok), tok)
    for i in range(n_arr):
        outs[i // 2][i % 2, :, my_cols] = ins[i][my_rows, :]
    for copy in copies:
        copy.wait()


def to_tokens(*arrs):
    seq_len, cols = arrs[0].shape
    tok = seq_len // N_DEV
    n_arr = len(arrs)
    outs = pl.pallas_call(
        functools.partial(to_tokens_kernel, n_arr, tok, cols),
        out_shape=[jax.ShapeDtypeStruct((2, tok, cols * N_DEV), jnp.bfloat16)] * (n_arr // 2),
        in_specs=[vmem_spec()] * n_arr,
        out_specs=[vmem_spec()] * (n_arr // 2),
        scratch_shapes=[pltpu.SemaphoreType.DMA((n_arr, N_DEV)), pltpu.SemaphoreType.DMA((n_arr, N_DEV))],
        compiler_params=pltpu.CompilerParams(has_side_effects=True),
        cost_estimate=pl.CostEstimate(flops=int(5e9) * n_arr, bytes_accessed=int(4e6) * n_arr, transcendentals=0),
        name='to_tokens',
    )(*arrs)
    return [o.reshape(2 * tok, cols * N_DEV) for o in outs]


def to_heads_kernel(tok, cols, in_ref, out0_ref, out1_ref, send_sems, recv_sems):
    me = lax.axis_index('tp')
    outs = (out0_ref, out1_ref)
    my_rows = pl.ds(pl.multiple_of(me * tok, tok), tok)
    copies = []
    for b in range(2):
        for step in range(1, N_DEV):
            peer = lax.rem(me + step, N_DEV)
            copy = pltpu.make_async_remote_copy(
                src_ref=in_ref.at[b, :, pl.ds(pl.multiple_of(peer * cols, cols), cols)], dst_ref=outs[b].at[my_rows, :],
                send_sem=send_sems.at[b, step], recv_sem=recv_sems.at[b, step],
                device_id=(peer,), device_id_type=pl.DeviceIdType.MESH)
            copy.start()
            copies.append(copy)
    for b in range(2):
        outs[b][my_rows, :] = in_ref[b, :, pl.ds(pl.multiple_of(me * cols, cols), cols)]
    for copy in copies:
        copy.wait()


def to_heads(arr):
    _, tok, width = arr.shape
    cols = width // N_DEV
    return pl.pallas_call(
        functools.partial(to_heads_kernel, tok, cols),
        out_shape=[jax.ShapeDtypeStruct((tok * N_DEV, cols), jnp.bfloat16)] * 2,
        in_specs=[vmem_spec()],
        out_specs=[vmem_spec()] * 2,
        scratch_shapes=[pltpu.SemaphoreType.DMA((2, N_DEV)), pltpu.SemaphoreType.DMA((2, N_DEV))],
        compiler_params=pltpu.CompilerParams(has_side_effects=True),
        cost_estimate=pl.CostEstimate(flops=int(1e10), bytes_accessed=int(8e6), transcendentals=0),
        name='to_heads',
    )(arr)


def causal_tile(scores, first_key_row):
    ext = scores.shape[0]
    diag = scores[first_key_row:, :]
    key_pos = lax.broadcasted_iota(jnp.int32, diag.shape, 0)
    query_pos = lax.broadcasted_iota(jnp.int32, diag.shape, 1)
    diag = jnp.where(key_pos <= query_pos, diag, -1e30)
    if first_key_row == 0:
        return diag
    return jnp.concatenate([scores[:first_key_row, :], diag], axis=0)


def fwd_kernel(q_ref, k_ref, v_ref, iq_ref, ik_ref, gq_ref, gk_ref, cos_ref, sin_ref,
               o_ref, qr_ref, kr_ref, lse_ref, vt_ref):
    seq_len = q_ref.shape[0]
    cos_t, sin_t = cos_ref[...], sin_ref[...]
    for src, inv, gain, dst in ((q_ref, iq_ref, gq_ref, qr_ref), (k_ref, ik_ref, gk_ref, kr_ref)):
        hat = src[...] * inv[...] * gain[...].astype(jnp.float32)
        dst[...] = (hat * cos_t + pltpu.roll(hat, HEAD_SIZE // 2, 1) * sin_t).astype(jnp.bfloat16)
    vt_ref[...] = v_ref[...].astype(jnp.float32).T.astype(jnp.bfloat16)
    for first in range(0, seq_len, Q_BLOCK):
        ext = first + Q_BLOCK
        scores = lax.dot_general(kr_ref[:ext, :], qr_ref[first:ext, :], NT,
                                 preferred_element_type=jnp.float32) * (ATTN_SCALE * LOG2E)
        scores = causal_tile(scores, first)
        top = jnp.max(scores, axis=0, keepdims=True)
        expd = jnp.exp2(scores - top)
        total = jnp.sum(expd, axis=0, keepdims=True)
        probs = (expd * (1.0 / total)).astype(jnp.bfloat16)
        out_t = lax.dot_general(vt_ref[:, :ext], probs, NN, preferred_element_type=jnp.float32)
        o_ref[first:ext, :] = out_t.T.astype(jnp.bfloat16)
        lse_ref[:, first:ext] = top + jnp.log2(total)


def attention_fwd(q_raw, k_raw, v_heads, inv_q, inv_k, gq, gk, cos_t, sin_t):
    seq_len, cols = q_raw.shape
    heads = cols // HEAD_SIZE
    head_spec = pl.BlockSpec((seq_len, HEAD_SIZE), lambda h: (0, h))
    col_spec = pl.BlockSpec((seq_len, 1), lambda h: (0, 0))
    gain_spec = pl.BlockSpec((1, HEAD_SIZE), lambda h: (0, h))
    table_spec = pl.BlockSpec((seq_len, HEAD_SIZE), lambda h: (0, 0))
    lse_spec = pl.BlockSpec((None, 1, seq_len), lambda h: (h, 0, 0))
    return pl.pallas_call(
        fwd_kernel,
        grid=(heads,),
        in_specs=[head_spec, head_spec, head_spec, col_spec, col_spec, gain_spec, gain_spec, table_spec, table_spec],
        out_specs=[head_spec, head_spec, head_spec, lse_spec],
        out_shape=[jax.ShapeDtypeStruct((seq_len, cols), jnp.bfloat16)] * 3
        + [jax.ShapeDtypeStruct((heads, 1, seq_len), jnp.float32)],
        scratch_shapes=[pltpu.VMEM((HEAD_SIZE, seq_len), jnp.bfloat16)],
        compiler_params=pltpu.CompilerParams(dimension_semantics=('arbitrary',), vmem_limit_bytes=56 * 2 ** 20),
        cost_estimate=pl.CostEstimate(flops=int(8e9), bytes_accessed=int(1e7), transcendentals=int(5e6)),
        name='attention_fwd',
    )(q_raw, k_raw, v_heads, inv_q, inv_k, gq, gk, cos_t, sin_t)


def bwd_kernel(q_ref, k_ref, v_ref, do_ref, lse_ref, cos_ref, sin_ref, dq_ref, dk_ref, dv_ref, kt_ref, dva_ref):
    seq_len = q_ref.shape[0]
    kt_ref[...] = k_ref[...].astype(jnp.float32).T.astype(jnp.bfloat16)
    dk_ref[...] = jnp.zeros_like(dk_ref)
    dva_ref[...] = jnp.zeros_like(dva_ref)
    for first in range(0, seq_len, Q_BLOCK):
        ext = first + Q_BLOCK
        q_blk, do_blk = q_ref[first:ext, :], do_ref[first:ext, :]
        scores = lax.dot_general(k_ref[:ext, :], q_blk, NT,
                                 preferred_element_type=jnp.float32) * (ATTN_SCALE * LOG2E)
        scores = causal_tile(scores, first)
        probs = jnp.exp2(scores - lse_ref[:, first:ext])
        d_probs = lax.dot_general(v_ref[:ext, :], do_blk, NT, preferred_element_type=jnp.float32)
        delta = jnp.sum(probs * d_probs, axis=0, keepdims=True)
        d_scores = (probs * (d_probs - delta) * ATTN_SCALE).astype(jnp.bfloat16)
        dva_ref[:ext, :] += lax.dot_general(probs.astype(jnp.bfloat16), do_blk, NN, preferred_element_type=jnp.float32)
        dk_ref[:ext, :] += lax.dot_general(d_scores, q_blk, NN, preferred_element_type=jnp.float32)
        dq_t = lax.dot_general(kt_ref[:, :ext], d_scores, NN, preferred_element_type=jnp.float32)
        dq = dq_t.T
        dq_ref[first:ext, :] = dq * cos_ref[first:ext, :] - pltpu.roll(dq, HEAD_SIZE // 2, 1) * sin_ref[first:ext, :]
    dk = dk_ref[...]
    dk_ref[...] = dk * cos_ref[...] - pltpu.roll(dk, HEAD_SIZE // 2, 1) * sin_ref[...]
    dv_ref[...] = dva_ref[...].astype(jnp.bfloat16)


def attention_bwd(q_rot, k_rot, v_heads, d_heads, lse, cos_t, sin_t):
    seq_len, cols = q_rot.shape
    heads = cols // HEAD_SIZE
    head_spec = pl.BlockSpec((seq_len, HEAD_SIZE), lambda h: (0, h))
    table_spec = pl.BlockSpec((seq_len, HEAD_SIZE), lambda h: (0, 0))
    lse_spec = pl.BlockSpec((None, 1, seq_len), lambda h: (h, 0, 0))
    return pl.pallas_call(
        bwd_kernel,
        grid=(heads,),
        in_specs=[head_spec, head_spec, head_spec, head_spec, lse_spec, table_spec, table_spec],
        out_specs=[head_spec, head_spec, head_spec],
        out_shape=[jax.ShapeDtypeStruct((seq_len, cols), jnp.float32)] * 2
        + [jax.ShapeDtypeStruct((seq_len, cols), jnp.bfloat16)],
        scratch_shapes=[pltpu.VMEM((HEAD_SIZE, seq_len), jnp.bfloat16), pltpu.VMEM((seq_len, HEAD_SIZE), jnp.float32)],
        compiler_params=pltpu.CompilerParams(dimension_semantics=('arbitrary',), vmem_limit_bytes=56 * 2 ** 20),
        cost_estimate=pl.CostEstimate(flops=int(2e10), bytes_accessed=int(1e7), transcendentals=int(5e6)),
        name='attention_bwd',
    )(q_rot, k_rot, v_heads, d_heads, lse, cos_t, sin_t)


def dot_f32(spec, lhs, rhs):
    return jnp.einsum(spec, lhs, rhs, preferred_element_type=jnp.float32)


def after(value, *others):
    return lax.optimization_barrier((value,) + others)[0]


def local_block(x_loc, wq_loc, wk_loc, wv_loc, wo_loc, gq_loc, gk_loc, g_attn, dy_loc):
    batch_size, seq_loc, model_dim = x_loc.shape
    seq_len = seq_loc * N_DEV
    batches = range(batch_size)
    cos_t, sin_t = rope_tables(seq_len)
    gq_row, gk_row = gq_loc[None, :], gk_loc[None, :]
    gq_f, gk_f = gq_row.astype(jnp.float32), gk_row.astype(jnp.float32)

    x_full = [lax.all_gather(x_loc[b], 'tp', axis=0, tiled=True) for b in batches]
    wo_full = lax.all_gather(wo_loc, 'tp', axis=0, tiled=True)
    wq_t, wk_t, wv_t = [lax.all_gather(w.T, 'tp', axis=0, tiled=True) for w in (wq_loc, wk_loc, wv_loc)]

    q_raw, k_raw, v_heads, inv_q, inv_k, saved = [], [], [], [], [], []
    for b in batches:
        q_b, k_b = dot_f32('sd,de->se', x_full[b], wq_loc), dot_f32('sd,de->se', x_full[b], wk_loc)
        part = jnp.stack([jnp.sum(q_b * q_b, axis=-1), jnp.sum(k_b * k_b, axis=-1)])
        v_b = dot_f32('sd,de->se', x_full[b], wv_loc).astype(jnp.bfloat16)
        sums = sum_devices(part.reshape(-1, 128)).reshape(2, seq_len, 1)
        inv = lax.rsqrt(sums / model_dim + NORM_EPS)
        saved.append(attention_fwd(q_b, k_b, v_b, inv[0], inv[1], gq_row, gk_row, cos_t, sin_t))
        q_raw.append(q_b)
        k_raw.append(k_b)
        v_heads.append(v_b)
        inv_q.append(inv[0])
        inv_k.append(inv[1])
    heads_out = [s[0] for s in saved]

    o_loc, = to_tokens(*heads_out)
    attn_loc = dot_f32('te,ed->td', o_loc, wo_full)
    x_f = x_loc.reshape(-1, model_dim).astype(jnp.float32)
    dy_f = dy_loc.reshape(-1, model_dim).astype(jnp.float32)
    post_rms = lax.rsqrt(jnp.mean(attn_loc * attn_loc, axis=-1, keepdims=True) + NORM_EPS)
    normed = attn_loc * post_rms
    ga_f = g_attn.astype(jnp.float32)
    y_loc = (x_f + normed * ga_f).astype(jnp.bfloat16)

    ga_part = jnp.sum(dy_f * normed, axis=0)
    g_normed = dy_f * ga_f
    d_attn = (post_rms * (g_normed - normed * jnp.mean(g_normed * normed, axis=-1, keepdims=True))).astype(jnp.bfloat16)
    d_o_loc = dot_f32('td,ed->te', d_attn, wo_full).astype(jnp.bfloat16)
    d_heads = to_heads(d_o_loc.reshape(batch_size, seq_loc, model_dim))
    d_attn_full = lax.all_gather(d_attn.reshape(batch_size, seq_loc, model_dim), 'tp', axis=1, tiled=True)

    dq_hat, dk_hat, d_value = [], [], []
    for b in batches:
        dq_b, dk_b, dv_b = attention_bwd(saved[b][1], saved[b][2], v_heads[b], d_heads[b], saved[b][3], cos_t, sin_t)
        dq_hat.append(dq_b)
        dk_hat.append(dk_b)
        d_value.append(dv_b)
    grad_wo = sum(dot_f32('se,sd->ed', heads_out[b], d_attn_full[b]) for b in batches)
    grad_gq = sum(jnp.sum(dq_hat[b] * (q_raw[b] * inv_q[b]), axis=0) for b in batches)
    grad_gk = sum(jnp.sum(dk_hat[b] * (k_raw[b] * inv_k[b]), axis=0) for b in batches)
    dots = [jnp.sum(dq_hat[b] * gq_f * (q_raw[b] * inv_q[b]), axis=-1) for b in batches]
    dots += [jnp.sum(dk_hat[b] * gk_f * (k_raw[b] * inv_k[b]), axis=-1) for b in batches]
    sums = sum_devices(jnp.concatenate(dots + [ga_part]).reshape(-1, 128)).reshape(-1)
    unit_dots = (sums[:2 * batch_size * seq_len] / model_dim).reshape(2, batch_size, seq_len, 1)
    grad_ga = sums[2 * batch_size * seq_len:]
    dq_raw = [(inv_q[b] * (dq_hat[b] * gq_f - q_raw[b] * inv_q[b] * unit_dots[0, b])).astype(jnp.bfloat16) for b in batches]
    dk_raw = [(inv_k[b] * (dk_hat[b] * gk_f - k_raw[b] * inv_k[b] * unit_dots[1, b])).astype(jnp.bfloat16) for b in batches]
    dq_loc, dk_loc, dv_loc = to_tokens(*dq_raw, *dk_raw, *d_value)
    grad_wq = sum(dot_f32('sd,se->de', x_full[b], dq_raw[b]) for b in batches)
    grad_wk = sum(dot_f32('sd,se->de', x_full[b], dk_raw[b]) for b in batches)
    grad_wv = sum(dot_f32('sd,se->de', x_full[b], d_value[b]) for b in batches)
    grad_x = (dot_f32('te,ed->td', dq_loc, wq_t) + dot_f32('te,ed->td', dk_loc, wk_t)
              + dot_f32('te,ed->td', dv_loc, wv_t) + dy_f)
    return (y_loc.reshape(x_loc.shape), grad_x.astype(jnp.bfloat16).reshape(x_loc.shape), grad_wq.astype(jnp.bfloat16),
            grad_wk.astype(jnp.bfloat16), grad_wv.astype(jnp.bfloat16), grad_wo.astype(jnp.bfloat16),
            grad_gq.astype(jnp.bfloat16), grad_gk.astype(jnp.bfloat16), grad_ga.astype(jnp.bfloat16))


def solution(mesh):
    act_spec = P(None, 'tp', None)
    col_spec = P(None, 'tp')
    row_spec = P('tp', None)
    vec_spec = P('tp')
    in_specs = (act_spec, col_spec, col_spec, col_spec, row_spec, vec_spec, vec_spec, P(), act_spec)
    out_specs = (act_spec, act_spec, col_spec, col_spec, col_spec, row_spec, vec_spec, vec_spec, P())
    return jax.shard_map(local_block, mesh=mesh, in_specs=in_specs, out_specs=out_specs, check_vma=False)
```

```python
import functools
import math

import jax
import jax.numpy as jnp
from jax import lax
from jax.experimental import pallas as pl
from jax.experimental.pallas import tpu as pltpu
from jax.sharding import PartitionSpec as P


HEAD_SIZE = 128
ROPE_THETA = 500000.0
NORM_EPS = 1e-6
N_DEV = 16
Q_BLOCK = 256
LOG2E = math.log2(math.e)
ATTN_SCALE = HEAD_SIZE ** -0.5
NT = (((1,), (1,)), ((), ()))
NN = (((1,), (0,)), ((), ()))


def rope_tables(seq_len):
    half_dim = HEAD_SIZE // 2
    inv_freq = 1.0 / (ROPE_THETA ** (jnp.arange(half_dim, dtype=jnp.float32) / half_dim))
    angles = jnp.arange(seq_len, dtype=jnp.float32)[:, None] * inv_freq[None, :]
    cos_t, sin_t = jnp.cos(angles), jnp.sin(angles)
    return jnp.concatenate([cos_t, cos_t], axis=-1), jnp.concatenate([-sin_t, sin_t], axis=-1)


def vmem_spec():
    return pl.BlockSpec(memory_space=pltpu.VMEM)


def sum_kernel(part_ref, out_ref, slots, send_sems, recv_sems):
    me = lax.axis_index('tp')
    copies = []
    for step in range(1, N_DEV):
        peer = lax.rem(me + step, N_DEV)
        copy = pltpu.make_async_remote_copy(
            src_ref=part_ref, dst_ref=slots.at[step], send_sem=send_sems.at[step], recv_sem=recv_sems.at[step],
            device_id=(peer,), device_id_type=pl.DeviceIdType.MESH)
        copy.start()
        copies.append(copy)
    slots[0] = part_ref[...]
    for copy in copies:
        copy.wait()
    total = jnp.zeros(part_ref.shape, jnp.float32)
    for owner in range(N_DEV):
        total = total + slots[lax.rem(me - owner + N_DEV, N_DEV)]
    out_ref[...] = total


def sum_devices(part):
    return pl.pallas_call(
        sum_kernel,
        out_shape=jax.ShapeDtypeStruct(part.shape, jnp.float32),
        in_specs=[vmem_spec()],
        out_specs=vmem_spec(),
        scratch_shapes=[pltpu.VMEM((N_DEV,) + part.shape, jnp.float32),
                        pltpu.SemaphoreType.DMA((N_DEV,)), pltpu.SemaphoreType.DMA((N_DEV,))],
        compiler_params=pltpu.CompilerParams(has_side_effects=True),
        cost_estimate=pl.CostEstimate(flops=int(1e9), bytes_accessed=int(1e6), transcendentals=0),
        name='sum_devices',
    )(part)


def to_tokens_kernel(n_arr, tok, cols, *refs):
    ins, outs = refs[:n_arr], refs[n_arr:-2]
    send_sems, recv_sems = refs[-2:]
    me = lax.axis_index('tp')
    copies = []
    my_cols = pl.ds(pl.multiple_of(me * cols, cols), cols)
    for step in range(1, N_DEV):
        peer = lax.rem(me + step, N_DEV)
        rows = pl.ds(pl.multiple_of(peer * tok, tok), tok)
        for i in range(n_arr):
            copy = pltpu.make_async_remote_copy(
                src_ref=ins[i].at[rows, :], dst_ref=outs[i // 2].at[i % 2, :, my_cols],
                send_sem=send_sems.at[i, step], recv_sem=recv_sems.at[i, step],
                device_id=(peer,), device_id_type=pl.DeviceIdType.MESH)
            copy.start()
            copies.append(copy)
    my_rows = pl.ds(pl.multiple_of(me * tok, tok), tok)
    for i in range(n_arr):
        outs[i // 2][i % 2, :, my_cols] = ins[i][my_rows, :]
    for copy in copies:
        copy.wait()


def to_tokens(*arrs):
    seq_len, cols = arrs[0].shape
    tok = seq_len // N_DEV
    n_arr = len(arrs)
    outs = pl.pallas_call(
        functools.partial(to_tokens_kernel, n_arr, tok, cols),
        out_shape=[jax.ShapeDtypeStruct((2, tok, cols * N_DEV), jnp.bfloat16)] * (n_arr // 2),
        in_specs=[vmem_spec()] * n_arr,
        out_specs=[vmem_spec()] * (n_arr // 2),
        scratch_shapes=[pltpu.SemaphoreType.DMA((n_arr, N_DEV)), pltpu.SemaphoreType.DMA((n_arr, N_DEV))],
        compiler_params=pltpu.CompilerParams(has_side_effects=True),
        cost_estimate=pl.CostEstimate(flops=int(5e9) * n_arr, bytes_accessed=int(4e6) * n_arr, transcendentals=0),
        name='to_tokens',
    )(*arrs)
    return [o.reshape(2 * tok, cols * N_DEV) for o in outs]


def to_heads_kernel(tok, cols, in_ref, out0_ref, out1_ref, send_sems, recv_sems):
    me = lax.axis_index('tp')
    outs = (out0_ref, out1_ref)
    my_rows = pl.ds(pl.multiple_of(me * tok, tok), tok)
    copies = []
    for b in range(2):
        for step in range(1, N_DEV):
            peer = lax.rem(me + step, N_DEV)
            copy = pltpu.make_async_remote_copy(
                src_ref=in_ref.at[b, :, pl.ds(pl.multiple_of(peer * cols, cols), cols)], dst_ref=outs[b].at[my_rows, :],
                send_sem=send_sems.at[b, step], recv_sem=recv_sems.at[b, step],
                device_id=(peer,), device_id_type=pl.DeviceIdType.MESH)
            copy.start()
            copies.append(copy)
    for b in range(2):
        outs[b][my_rows, :] = in_ref[b, :, pl.ds(pl.multiple_of(me * cols, cols), cols)]
    for copy in copies:
        copy.wait()


def to_heads(arr):
    _, tok, width = arr.shape
    cols = width // N_DEV
    return pl.pallas_call(
        functools.partial(to_heads_kernel, tok, cols),
        out_shape=[jax.ShapeDtypeStruct((tok * N_DEV, cols), jnp.bfloat16)] * 2,
        in_specs=[vmem_spec()],
        out_specs=[vmem_spec()] * 2,
        scratch_shapes=[pltpu.SemaphoreType.DMA((2, N_DEV)), pltpu.SemaphoreType.DMA((2, N_DEV))],
        compiler_params=pltpu.CompilerParams(has_side_effects=True),
        cost_estimate=pl.CostEstimate(flops=int(1e10), bytes_accessed=int(8e6), transcendentals=0),
        name='to_heads',
    )(arr)


def causal_tile(scores, first_key_row):
    diag = scores[first_key_row:, :]
    key_pos = lax.broadcasted_iota(jnp.int32, diag.shape, 0)
    query_pos = lax.broadcasted_iota(jnp.int32, diag.shape, 1)
    diag = jnp.where(key_pos <= query_pos, diag, -1e30)
    if first_key_row == 0:
        return diag
    return jnp.concatenate([scores[:first_key_row, :], diag], axis=0)


def fwd_kernel(q_ref, k_ref, v_ref, iq_ref, ik_ref, gq_ref, gk_ref, cos_ref, sin_ref,
               o_ref, qr_ref, kr_ref, lse_ref, vt_ref):
    seq_len = q_ref.shape[0]
    cos_t, sin_t = cos_ref[...], sin_ref[...]
    for src, inv, gain, dst in ((q_ref, iq_ref, gq_ref, qr_ref), (k_ref, ik_ref, gk_ref, kr_ref)):
        hat = src[...] * inv[...] * gain[...].astype(jnp.float32)
        dst[...] = (hat * cos_t + pltpu.roll(hat, HEAD_SIZE // 2, 1) * sin_t).astype(jnp.bfloat16)
    vt_ref[...] = v_ref[...].astype(jnp.float32).T.astype(jnp.bfloat16)
    for first in range(0, seq_len, Q_BLOCK):
        ext = first + Q_BLOCK
        scores = lax.dot_general(kr_ref[:ext, :], qr_ref[first:ext, :], NT,
                                 preferred_element_type=jnp.float32) * (ATTN_SCALE * LOG2E)
        scores = causal_tile(scores, first)
        top = jnp.max(scores, axis=0, keepdims=True)
        expd = jnp.exp2(scores - top)
        total = jnp.sum(expd, axis=0, keepdims=True)
        probs = (expd * (1.0 / total)).astype(jnp.bfloat16)
        out_t = lax.dot_general(vt_ref[:, :ext], probs, NN, preferred_element_type=jnp.float32)
        o_ref[first:ext, :] = out_t.T.astype(jnp.bfloat16)
        lse_ref[:, first:ext] = top + jnp.log2(total)


def attention_fwd(q_raw, k_raw, v_heads, inv_q, inv_k, gq, gk, cos_t, sin_t):
    seq_len, cols = q_raw.shape
    heads = cols // HEAD_SIZE
    head_spec = pl.BlockSpec((seq_len, HEAD_SIZE), lambda h: (0, h))
    col_spec = pl.BlockSpec((seq_len, 1), lambda h: (0, 0))
    gain_spec = pl.BlockSpec((1, HEAD_SIZE), lambda h: (0, h))
    table_spec = pl.BlockSpec((seq_len, HEAD_SIZE), lambda h: (0, 0))
    lse_spec = pl.BlockSpec((None, 1, seq_len), lambda h: (h, 0, 0))
    return pl.pallas_call(
        fwd_kernel,
        grid=(heads,),
        in_specs=[head_spec, head_spec, head_spec, col_spec, col_spec, gain_spec, gain_spec, table_spec, table_spec],
        out_specs=[head_spec, head_spec, head_spec, lse_spec],
        out_shape=[jax.ShapeDtypeStruct((seq_len, cols), jnp.bfloat16)] * 3
        + [jax.ShapeDtypeStruct((heads, 1, seq_len), jnp.float32)],
        scratch_shapes=[pltpu.VMEM((HEAD_SIZE, seq_len), jnp.bfloat16)],
        compiler_params=pltpu.CompilerParams(dimension_semantics=('arbitrary',), vmem_limit_bytes=56 * 2 ** 20),
        cost_estimate=pl.CostEstimate(flops=int(8e9), bytes_accessed=int(1e7), transcendentals=int(5e6)),
        name='attention_fwd',
    )(q_raw, k_raw, v_heads, inv_q, inv_k, gq, gk, cos_t, sin_t)


def bwd_kernel(q_ref, k_ref, v_ref, do_ref, lse_ref, cos_ref, sin_ref, dq_ref, dk_ref, dv_ref, kt_ref, dva_ref):
    seq_len = q_ref.shape[0]
    kt_ref[...] = k_ref[...].astype(jnp.float32).T.astype(jnp.bfloat16)
    dk_ref[...] = jnp.zeros_like(dk_ref)
    dva_ref[...] = jnp.zeros_like(dva_ref)
    for first in range(0, seq_len, Q_BLOCK):
        ext = first + Q_BLOCK
        q_blk, do_blk = q_ref[first:ext, :], do_ref[first:ext, :]
        scores = lax.dot_general(k_ref[:ext, :], q_blk, NT,
                                 preferred_element_type=jnp.float32) * (ATTN_SCALE * LOG2E)
        scores = causal_tile(scores, first)
        probs = jnp.exp2(scores - lse_ref[:, first:ext])
        d_probs = lax.dot_general(v_ref[:ext, :], do_blk, NT, preferred_element_type=jnp.float32)
        delta = jnp.sum(probs * d_probs, axis=0, keepdims=True)
        d_scores = (probs * (d_probs - delta) * ATTN_SCALE).astype(jnp.bfloat16)
        dva_ref[:ext, :] += lax.dot_general(probs.astype(jnp.bfloat16), do_blk, NN, preferred_element_type=jnp.float32)
        dk_ref[:ext, :] += lax.dot_general(d_scores, q_blk, NN, preferred_element_type=jnp.float32)
        dq_t = lax.dot_general(kt_ref[:, :ext], d_scores, NN, preferred_element_type=jnp.float32)
        dq = dq_t.T
        dq_ref[first:ext, :] = dq * cos_ref[first:ext, :] - pltpu.roll(dq, HEAD_SIZE // 2, 1) * sin_ref[first:ext, :]
    dk = dk_ref[...]
    dk_ref[...] = dk * cos_ref[...] - pltpu.roll(dk, HEAD_SIZE // 2, 1) * sin_ref[...]
    dv_ref[...] = dva_ref[...].astype(jnp.bfloat16)


def attention_bwd(q_rot, k_rot, v_heads, d_heads, lse, cos_t, sin_t):
    seq_len, cols = q_rot.shape
    heads = cols // HEAD_SIZE
    head_spec = pl.BlockSpec((seq_len, HEAD_SIZE), lambda h: (0, h))
    table_spec = pl.BlockSpec((seq_len, HEAD_SIZE), lambda h: (0, 0))
    lse_spec = pl.BlockSpec((None, 1, seq_len), lambda h: (h, 0, 0))
    return pl.pallas_call(
        bwd_kernel,
        grid=(heads,),
        in_specs=[head_spec, head_spec, head_spec, head_spec, lse_spec, table_spec, table_spec],
        out_specs=[head_spec, head_spec, head_spec],
        out_shape=[jax.ShapeDtypeStruct((seq_len, cols), jnp.float32)] * 2
        + [jax.ShapeDtypeStruct((seq_len, cols), jnp.bfloat16)],
        scratch_shapes=[pltpu.VMEM((HEAD_SIZE, seq_len), jnp.bfloat16), pltpu.VMEM((seq_len, HEAD_SIZE), jnp.float32)],
        compiler_params=pltpu.CompilerParams(dimension_semantics=('arbitrary',), vmem_limit_bytes=56 * 2 ** 20),
        cost_estimate=pl.CostEstimate(flops=int(2e10), bytes_accessed=int(1e7), transcendentals=int(5e6)),
        name='attention_bwd',
    )(q_rot, k_rot, v_heads, d_heads, lse, cos_t, sin_t)


COLUMN_PARTS = ((0, 1408), (1408, 2816), (2816, 4096))
AXIS_ORDERS = ((0, 1, 2), (1, 2, 0), (2, 0, 1))


def by_distance_kernel(me_ref, dq_ref, dk_ref, dv_ref, out_ref):
    cols = dq_ref.shape[-1]
    for i, ref in enumerate((dq_ref, dk_ref, dv_ref)):
        out_ref[:, i * cols:(i + 1) * cols] = ref[...]


def by_distance(dq, dk, dv):
    seq_len, cols = dq.shape
    tok = seq_len // N_DEV
    in_spec = pl.BlockSpec((tok, cols), lambda i, me: (((i % 8) * 2 + i // 8) ^ me[0], 0))
    out = pl.pallas_call(
        by_distance_kernel,
        grid_spec=pltpu.PrefetchScalarGridSpec(
            num_scalar_prefetch=1, grid=(N_DEV,), in_specs=[in_spec] * 3,
            out_specs=pl.BlockSpec((tok, 3 * cols), lambda i, me: (i, 0))),
        out_shape=jax.ShapeDtypeStruct((seq_len, 3 * cols), jnp.bfloat16),
        cost_estimate=pl.CostEstimate(flops=int(1e9), bytes_accessed=int(6e6), transcendentals=0),
        name='by_distance',
    )(lax.axis_index('tp').astype(jnp.int32).reshape(1), dq, dk, dv)
    return out[seq_len // 2:], out[:seq_len // 2]


def flip(value, bit):
    return lax.ppermute(value, 'tp', [(i, i ^ bit) for i in range(N_DEV)])


def start_sums(far, near):
    shape = (2, 2, 2, near[0].shape[0] // 8)
    return [[n.reshape(shape + n.shape[1:]), flip(f, 1).reshape(shape + n.shape[1:])] for f, n in zip(far, near)]


def cross_axis(sums, stage):
    aways, kept = [], []
    for pieces, order in zip(sums, AXIS_ORDERS):
        axis = order[stage]
        away = sum(lax.slice_in_dim(p, 1, 2, axis=axis) for p in pieces)
        aways.append(away)
        came = flip(away, 8 >> axis)
        kept.append([sum(lax.slice_in_dim(p, 0, 1, axis=axis) for p in pieces), came])
    return kept, aways


def sums_after(sums, gate):
    flat = lax.optimization_barrier(tuple(p for pieces in sums for p in pieces) + tuple(gate))
    size = len(sums[0])
    return [list(flat[i * size:(i + 1) * size]) for i in range(len(sums))]


def finish_sums(sums):
    return jnp.concatenate([sum(pieces)[0, 0, 0] for pieces in sums], axis=-1)


def dot_f32(spec, lhs, rhs):
    return jnp.einsum(spec, lhs, rhs, preferred_element_type=jnp.float32)


def after(value, *others):
    return lax.optimization_barrier((value,) + others)[0]


def local_block(x_loc, wq_loc, wk_loc, wv_loc, wo_loc, gq_loc, gk_loc, g_attn, dy_loc):
    batch_size, seq_loc, model_dim = x_loc.shape
    seq_len = seq_loc * N_DEV
    batches = range(batch_size)
    cos_t, sin_t = rope_tables(seq_len)
    gq_row, gk_row = gq_loc[None, :], gk_loc[None, :]
    gq_f, gk_f = gq_row.astype(jnp.float32), gk_row.astype(jnp.float32)

    x_full = [lax.all_gather(x_loc[b], 'tp', axis=0, tiled=True) for b in batches]
    wo_full = lax.all_gather(wo_loc, 'tp', axis=0, tiled=True)
    w_cat = jnp.concatenate([wq_loc, wk_loc, wv_loc], axis=1)

    q_raw, k_raw, v_heads, inv_q, inv_k, saved = [], [], [], [], [], []
    for b in batches:
        x_full[b] = after(x_full[b], saved[b - 1][0] if b else w_cat)
        q_b, k_b = dot_f32('sd,de->se', x_full[b], wq_loc), dot_f32('sd,de->se', x_full[b], wk_loc)
        part = jnp.stack([jnp.sum(q_b * q_b, axis=-1), jnp.sum(k_b * k_b, axis=-1)])
        v_b = dot_f32('sd,de->se', x_full[b], wv_loc).astype(jnp.bfloat16)
        sums = sum_devices(after(part.reshape(-1, 128), v_b)).reshape(2, seq_len, 1)
        inv = lax.rsqrt(sums / model_dim + NORM_EPS)
        saved.append(attention_fwd(q_b, k_b, v_b, inv[0], inv[1], gq_row, gk_row, cos_t, sin_t))
        q_raw.append(q_b)
        k_raw.append(k_b)
        v_heads.append(v_b)
        inv_q.append(inv[0])
        inv_k.append(inv[1])
    heads_out = [s[0] for s in saved]

    o_loc, = to_tokens(*heads_out)
    attn_loc = dot_f32('te,ed->td', o_loc, wo_full)
    x_f = x_loc.reshape(-1, model_dim).astype(jnp.float32)
    dy_f = dy_loc.reshape(-1, model_dim).astype(jnp.float32)
    post_rms = lax.rsqrt(jnp.mean(attn_loc * attn_loc, axis=-1, keepdims=True) + NORM_EPS)
    normed = attn_loc * post_rms
    ga_f = g_attn.astype(jnp.float32)
    y_loc = (x_f + normed * ga_f).astype(jnp.bfloat16)

    ga_part = jnp.sum(dy_f * normed, axis=0)
    g_normed = dy_f * ga_f
    d_attn = (post_rms * (g_normed - normed * jnp.mean(g_normed * normed, axis=-1, keepdims=True))).astype(jnp.bfloat16)
    d_o_loc = dot_f32('td,ed->te', d_attn, wo_full).astype(jnp.bfloat16)
    d_heads = to_heads(d_o_loc.reshape(batch_size, seq_loc, model_dim))
    d_attn_full = lax.all_gather(d_attn.reshape(batch_size, seq_loc, model_dim), 'tp', axis=1, tiled=True)

    dq_raw, dk_raw, d_value, dx_sums, gate = [], [], [], [], []
    grad_gq, grad_gk = 0.0, 0.0
    for b in batches:
        dq_b, dk_b, dv_b = attention_bwd(saved[b][1], saved[b][2], v_heads[b], after(d_heads[b], *gate),
                                         saved[b][3], cos_t, sin_t)
        q_unit, k_unit = q_raw[b] * inv_q[b], k_raw[b] * inv_k[b]
        dq_unit, dk_unit = dq_b * gq_f, dk_b * gk_f
        grad_gq += jnp.sum(dq_b * q_unit, axis=0)
        grad_gk += jnp.sum(dk_b * k_unit, axis=0)
        parts = [jnp.sum(dq_unit * q_unit, axis=-1), jnp.sum(dk_unit * k_unit, axis=-1)]
        if b == 0:
            parts.append(ga_part)
        sums = sum_devices(jnp.concatenate(parts).reshape(-1, 128)).reshape(-1)
        if b == 0:
            grad_ga = sums[2 * seq_len:]
        unit_dots = (sums[:2 * seq_len] / model_dim).reshape(2, seq_len, 1)
        dq_raw.append((inv_q[b] * (dq_unit - q_unit * unit_dots[0])).astype(jnp.bfloat16))
        dk_raw.append((inv_k[b] * (dk_unit - k_unit * unit_dots[1])).astype(jnp.bfloat16))
        d_value.append(dv_b)
        far, near = by_distance(dq_raw[b], dk_raw[b], dv_b)
        far_parts = [dot_f32('te,de->td', far, w_cat[lo:hi]) for lo, hi in COLUMN_PARTS]
        near_parts = [dot_f32('te,de->td', near, w_cat[lo:hi]) for lo, hi in COLUMN_PARTS]
        sums_b = start_sums(far_parts, near_parts)
        if b == 0:
            sums_b, gate = cross_axis(sums_b, 0)
        dx_sums.append(sums_b)
    dx_sums[0], gate = cross_axis(dx_sums[0], 1)
    dx_sums[1], gate = cross_axis(sums_after(dx_sums[1], gate), 0)
    first_grads = [dot_f32('sd,se->de', after(x_full[0], *gate), cot[0]) for cot in (dq_raw, dk_raw, d_value)]
    x_last = after(x_full[1], *first_grads)
    weight_grads = [(g + dot_f32('sd,se->de', x_last, cot[1])).astype(jnp.bfloat16)
                    for g, cot in zip(first_grads, (dq_raw, dk_raw, d_value))]
    d_attn_full = after(d_attn_full, *weight_grads)
    grad_wo = sum(dot_f32('se,sd->ed', heads_out[b], d_attn_full[b]) for b in batches).astype(jnp.bfloat16)
    dx_sums[1], gate = cross_axis(sums_after(dx_sums[1], [grad_wo]), 1)
    dx_sums[0], gate = cross_axis(sums_after(dx_sums[0], gate), 2)
    dx_sums[1], _ = cross_axis(sums_after(dx_sums[1], gate), 2)
    grad_x = jnp.stack([finish_sums(dx_sums[b]) + dy_loc[b].astype(jnp.float32) for b in batches])
    return (y_loc.reshape(x_loc.shape), grad_x.astype(jnp.bfloat16), *weight_grads, grad_wo,
            grad_gq.astype(jnp.bfloat16), grad_gk.astype(jnp.bfloat16), grad_ga.astype(jnp.bfloat16))


def solution(mesh):
    act_spec = P(None, 'tp', None)
    col_spec = P(None, 'tp')
    row_spec = P('tp', None)
    vec_spec = P('tp')
    in_specs = (act_spec, col_spec, col_spec, col_spec, row_spec, vec_spec, vec_spec, P(), act_spec)
    out_specs = (act_spec, act_spec, col_spec, col_spec, col_spec, row_spec, vec_spec, vec_spec, P())

    return jax.shard_map(local_block, mesh=mesh, in_specs=in_specs, out_specs=out_specs, check_vma=False)
```

```python
import functools
import math

import jax
import jax.numpy as jnp
from jax import lax
from jax.experimental import pallas as pl
from jax.experimental.pallas import tpu as pltpu
from jax.sharding import PartitionSpec as P


HEAD_SIZE = 128
ROPE_THETA = 500000.0
NORM_EPS = 1e-6
N_DEV = 16
Q_BLOCK = 256
LOG2E = math.log2(math.e)
ATTN_SCALE = HEAD_SIZE ** -0.5
NT = (((1,), (1,)), ((), ()))
NN = (((1,), (0,)), ((), ()))


def rope_tables(seq_len):
    half_dim = HEAD_SIZE // 2
    inv_freq = 1.0 / (ROPE_THETA ** (jnp.arange(half_dim, dtype=jnp.float32) / half_dim))
    angles = jnp.arange(seq_len, dtype=jnp.float32)[:, None] * inv_freq[None, :]
    cos_t, sin_t = jnp.cos(angles), jnp.sin(angles)
    return jnp.concatenate([cos_t, cos_t], axis=-1), jnp.concatenate([-sin_t, sin_t], axis=-1)


def vmem_spec():
    return pl.BlockSpec(memory_space=pltpu.VMEM)


def sum_kernel(part_ref, out_ref, slots, send_sems, recv_sems):
    me = lax.axis_index('tp')
    copies = []
    for step in range(1, N_DEV):
        peer = lax.rem(me + step, N_DEV)
        copy = pltpu.make_async_remote_copy(
            src_ref=part_ref, dst_ref=slots.at[step], send_sem=send_sems.at[step], recv_sem=recv_sems.at[step],
            device_id=(peer,), device_id_type=pl.DeviceIdType.MESH)
        copy.start()
        copies.append(copy)
    slots[0] = part_ref[...]
    for copy in copies:
        copy.wait()
    total = jnp.zeros(part_ref.shape, jnp.float32)
    for owner in range(N_DEV):
        total = total + slots[lax.rem(me - owner + N_DEV, N_DEV)]
    out_ref[...] = total


def sum_devices(part):
    return pl.pallas_call(
        sum_kernel,
        out_shape=jax.ShapeDtypeStruct(part.shape, jnp.float32),
        in_specs=[vmem_spec()],
        out_specs=vmem_spec(),
        scratch_shapes=[pltpu.VMEM((N_DEV,) + part.shape, jnp.float32),
                        pltpu.SemaphoreType.DMA((N_DEV,)), pltpu.SemaphoreType.DMA((N_DEV,))],
        compiler_params=pltpu.CompilerParams(has_side_effects=True),
        cost_estimate=pl.CostEstimate(flops=int(1e9), bytes_accessed=int(1e6), transcendentals=0),
        name='sum_devices',
    )(part)


def to_tokens_kernel(tok, cols, in_ref, out_ref, send_sems, recv_sems):
    me = lax.axis_index('tp')
    copies = []
    my_cols = pl.ds(pl.multiple_of(me * cols, cols), cols)
    for step in range(1, N_DEV):
        peer = lax.rem(me + step, N_DEV)
        copy = pltpu.make_async_remote_copy(
            src_ref=in_ref.at[:, pl.ds(pl.multiple_of(peer * tok, tok), tok), :], dst_ref=out_ref.at[:, :, my_cols],
            send_sem=send_sems.at[step], recv_sem=recv_sems.at[step],
            device_id=(peer,), device_id_type=pl.DeviceIdType.MESH)
        copy.start()
        copies.append(copy)
    out_ref[:, :, my_cols] = in_ref[:, pl.ds(pl.multiple_of(me * tok, tok), tok), :]
    for copy in copies:
        copy.wait()


def to_heads_kernel(tok, cols, in_ref, out_ref, send_sems, recv_sems):
    me = lax.axis_index('tp')
    my_rows = pl.ds(pl.multiple_of(me * tok, tok), tok)
    copies = []
    for step in range(1, N_DEV):
        peer = lax.rem(me + step, N_DEV)
        copy = pltpu.make_async_remote_copy(
            src_ref=in_ref.at[:, :, pl.ds(pl.multiple_of(peer * cols, cols), cols)], dst_ref=out_ref.at[:, my_rows, :],
            send_sem=send_sems.at[step], recv_sem=recv_sems.at[step],
            device_id=(peer,), device_id_type=pl.DeviceIdType.MESH)
        copy.start()
        copies.append(copy)
    out_ref[:, my_rows, :] = in_ref[:, :, pl.ds(pl.multiple_of(me * cols, cols), cols)]
    for copy in copies:
        copy.wait()


def exchange(kernel, arr, tok, cols, out_shape):
    return pl.pallas_call(
        functools.partial(kernel, tok, cols),
        out_shape=jax.ShapeDtypeStruct(out_shape, jnp.bfloat16),
        in_specs=[vmem_spec()],
        out_specs=vmem_spec(),
        scratch_shapes=[pltpu.SemaphoreType.DMA((N_DEV,)), pltpu.SemaphoreType.DMA((N_DEV,))],
        compiler_params=pltpu.CompilerParams(has_side_effects=True),
        cost_estimate=pl.CostEstimate(flops=int(1e10), bytes_accessed=int(8e6), transcendentals=0),
    )(arr)


def to_tokens(arr):
    batch_size, seq_len, cols = arr.shape
    tok = seq_len // N_DEV
    return exchange(to_tokens_kernel, arr, tok, cols, (batch_size, tok, cols * N_DEV))


def to_heads(arr):
    batch_size, tok, width = arr.shape
    cols = width // N_DEV
    return exchange(to_heads_kernel, arr, tok, cols, (batch_size, tok * N_DEV, cols))


def causal_tile(scores, first_key_row):
    diag = scores[first_key_row:, :]
    key_pos = lax.broadcasted_iota(jnp.int32, diag.shape, 0)
    query_pos = lax.broadcasted_iota(jnp.int32, diag.shape, 1)
    diag = jnp.where(key_pos <= query_pos, diag, -1e30)
    if first_key_row == 0:
        return diag
    return jnp.concatenate([scores[:first_key_row, :], diag], axis=0)


def fwd_kernel(q_ref, k_ref, v_ref, iq_ref, ik_ref, gq_ref, gk_ref, cos_ref, sin_ref,
               o_ref, qr_ref, kr_ref, lse_ref, vt_ref):
    seq_len = q_ref.shape[0]
    cos_t, sin_t = cos_ref[...], sin_ref[...]
    for src, inv, gain, dst in ((q_ref, iq_ref, gq_ref, qr_ref), (k_ref, ik_ref, gk_ref, kr_ref)):
        hat = src[...] * inv[...] * gain[...].astype(jnp.float32)
        dst[...] = (hat * cos_t + pltpu.roll(hat, HEAD_SIZE // 2, 1) * sin_t).astype(jnp.bfloat16)
    vt_ref[...] = v_ref[...].astype(jnp.float32).T.astype(jnp.bfloat16)
    for first in range(0, seq_len, Q_BLOCK):
        ext = first + Q_BLOCK
        scores = lax.dot_general(kr_ref[:ext, :], qr_ref[first:ext, :], NT,
                                 preferred_element_type=jnp.float32) * (ATTN_SCALE * LOG2E)
        scores = causal_tile(scores, first)
        top = jnp.max(scores, axis=0, keepdims=True)
        expd = jnp.exp2(scores - top)
        total = jnp.sum(expd, axis=0, keepdims=True)
        probs = (expd * (1.0 / total)).astype(jnp.bfloat16)
        out_t = lax.dot_general(vt_ref[:, :ext], probs, NN, preferred_element_type=jnp.float32)
        o_ref[first:ext, :] = out_t.T.astype(jnp.bfloat16)
        lse_ref[:, first:ext] = top + jnp.log2(total)


def attention_fwd(q_raw, k_raw, v_heads, inv_q, inv_k, gq, gk, cos_t, sin_t):
    batch_size, seq_len, cols = q_raw.shape
    heads = cols // HEAD_SIZE
    head_spec = pl.BlockSpec((None, seq_len, HEAD_SIZE), lambda b, h: (b, 0, h))
    col_spec = pl.BlockSpec((None, seq_len, 1), lambda b, h: (b, 0, 0))
    gain_spec = pl.BlockSpec((1, HEAD_SIZE), lambda b, h: (0, h))
    table_spec = pl.BlockSpec((seq_len, HEAD_SIZE), lambda b, h: (0, 0))
    lse_spec = pl.BlockSpec((None, None, 1, seq_len), lambda b, h: (b, h, 0, 0))
    return pl.pallas_call(
        fwd_kernel,
        grid=(batch_size, heads),
        in_specs=[head_spec, head_spec, head_spec, col_spec, col_spec, gain_spec, gain_spec, table_spec, table_spec],
        out_specs=[head_spec, head_spec, head_spec, lse_spec],
        out_shape=[jax.ShapeDtypeStruct((batch_size, seq_len, cols), jnp.bfloat16)] * 3
        + [jax.ShapeDtypeStruct((batch_size, heads, 1, seq_len), jnp.float32)],
        scratch_shapes=[pltpu.VMEM((HEAD_SIZE, seq_len), jnp.bfloat16)],
        compiler_params=pltpu.CompilerParams(dimension_semantics=('arbitrary', 'arbitrary'), vmem_limit_bytes=56 * 2 ** 20),
        cost_estimate=pl.CostEstimate(flops=int(8e9), bytes_accessed=int(1e7), transcendentals=int(5e6)),
        name='attention_fwd',
    )(q_raw, k_raw, v_heads, inv_q, inv_k, gq, gk, cos_t, sin_t)


def bwd_kernel(q_ref, k_ref, v_ref, do_ref, lse_ref, cos_ref, sin_ref, dq_ref, dk_ref, dv_ref, kt_ref, dva_ref):
    seq_len = q_ref.shape[0]
    kt_ref[...] = k_ref[...].astype(jnp.float32).T.astype(jnp.bfloat16)
    dk_ref[...] = jnp.zeros_like(dk_ref)
    dva_ref[...] = jnp.zeros_like(dva_ref)
    for first in range(0, seq_len, Q_BLOCK):
        ext = first + Q_BLOCK
        q_blk, do_blk = q_ref[first:ext, :], do_ref[first:ext, :]
        scores = lax.dot_general(k_ref[:ext, :], q_blk, NT,
                                 preferred_element_type=jnp.float32) * (ATTN_SCALE * LOG2E)
        scores = causal_tile(scores, first)
        probs = jnp.exp2(scores - lse_ref[:, first:ext])
        d_probs = lax.dot_general(v_ref[:ext, :], do_blk, NT, preferred_element_type=jnp.float32)
        delta = jnp.sum(probs * d_probs, axis=0, keepdims=True)
        d_scores = (probs * (d_probs - delta) * ATTN_SCALE).astype(jnp.bfloat16)
        dva_ref[:ext, :] += lax.dot_general(probs.astype(jnp.bfloat16), do_blk, NN, preferred_element_type=jnp.float32)
        dk_ref[:ext, :] += lax.dot_general(d_scores, q_blk, NN, preferred_element_type=jnp.float32)
        dq_t = lax.dot_general(kt_ref[:, :ext], d_scores, NN, preferred_element_type=jnp.float32)
        dq = dq_t.T
        dq_ref[first:ext, :] = dq * cos_ref[first:ext, :] - pltpu.roll(dq, HEAD_SIZE // 2, 1) * sin_ref[first:ext, :]
    dk = dk_ref[...]
    dk_ref[...] = dk * cos_ref[...] - pltpu.roll(dk, HEAD_SIZE // 2, 1) * sin_ref[...]
    dv_ref[...] = dva_ref[...].astype(jnp.bfloat16)


def attention_bwd(q_rot, k_rot, v_heads, d_heads, lse, cos_t, sin_t):
    batch_size, seq_len, cols = q_rot.shape
    heads = cols // HEAD_SIZE
    head_spec = pl.BlockSpec((None, seq_len, HEAD_SIZE), lambda b, h: (b, 0, h))
    table_spec = pl.BlockSpec((seq_len, HEAD_SIZE), lambda b, h: (0, 0))
    lse_spec = pl.BlockSpec((None, None, 1, seq_len), lambda b, h: (b, h, 0, 0))
    return pl.pallas_call(
        bwd_kernel,
        grid=(batch_size, heads),
        in_specs=[head_spec, head_spec, head_spec, head_spec, lse_spec, table_spec, table_spec],
        out_specs=[head_spec, head_spec, head_spec],
        out_shape=[jax.ShapeDtypeStruct((batch_size, seq_len, cols), jnp.float32)] * 2
        + [jax.ShapeDtypeStruct((batch_size, seq_len, cols), jnp.bfloat16)],
        scratch_shapes=[pltpu.VMEM((HEAD_SIZE, seq_len), jnp.bfloat16), pltpu.VMEM((seq_len, HEAD_SIZE), jnp.float32)],
        compiler_params=pltpu.CompilerParams(dimension_semantics=('arbitrary', 'arbitrary'), vmem_limit_bytes=56 * 2 ** 20),
        cost_estimate=pl.CostEstimate(flops=int(2e10), bytes_accessed=int(1e7), transcendentals=int(5e6)),
        name='attention_bwd',
    )(q_rot, k_rot, v_heads, d_heads, lse, cos_t, sin_t)


COLUMN_PARTS = ((0, 1408), (1408, 2816), (2816, 4096))
AXIS_ORDERS = ((0, 1, 2), (1, 2, 0), (2, 0, 1))


def by_distance_kernel(tok, cols, dq_ref, dk_ref, dv_ref, *out_refs):
    me = lax.axis_index('tp')
    for b in range(2):
        for side in range(2):
            for chip in range(N_DEV // 2):
                owner = (2 * chip + 1 - side) ^ me
                rows = pl.ds(pl.multiple_of(owner * tok, tok), tok)
                for i, ref in enumerate((dq_ref, dk_ref, dv_ref)):
                    out_refs[2 * b + side][chip * tok:(chip + 1) * tok, i * cols:(i + 1) * cols] = ref[b, rows, :]


def by_distance(dq, dk, dv):
    _, seq_len, cols = dq.shape
    far_0, near_0, far_1, near_1 = pl.pallas_call(
        functools.partial(by_distance_kernel, seq_len // N_DEV, cols),
        in_specs=[vmem_spec()] * 3,
        out_specs=[vmem_spec()] * 4,
        out_shape=[jax.ShapeDtypeStruct((seq_len // 2, 3 * cols), jnp.bfloat16)] * 4,
        compiler_params=pltpu.CompilerParams(vmem_limit_bytes=40 * 2 ** 20),
        cost_estimate=pl.CostEstimate(flops=int(1e9), bytes_accessed=int(12e6), transcendentals=0),
        name='by_distance',
    )(dq, dk, dv)
    return (far_0, far_1), (near_0, near_1)


def flip(value, bit):
    return lax.ppermute(value, 'tp', [(i, i ^ bit) for i in range(N_DEV)])


def start_sums(far, near):
    shape = (2, 2, 2, near[0].shape[0] // 8)
    return [[n.reshape(shape + n.shape[1:]), flip(f, 1).reshape(shape + n.shape[1:])] for f, n in zip(far, near)]


def cross_axis(sums, stage):
    aways, kept = [], []
    for pieces, order in zip(sums, AXIS_ORDERS):
        axis = order[stage]
        away = sum(lax.slice_in_dim(p, 1, 2, axis=axis) for p in pieces)
        aways.append(away)
        came = flip(away, 8 >> axis)
        kept.append([sum(lax.slice_in_dim(p, 0, 1, axis=axis) for p in pieces), came])
    return kept, aways


def sums_after(sums, gate):
    flat = lax.optimization_barrier(tuple(p for pieces in sums for p in pieces) + tuple(gate))
    size = len(sums[0])
    return [list(flat[i * size:(i + 1) * size]) for i in range(len(sums))]


def finish_sums(sums):
    return jnp.concatenate([sum(pieces)[0, 0, 0] for pieces in sums], axis=-1)


def dot_f32(spec, lhs, rhs):
    return jnp.einsum(spec, lhs, rhs, preferred_element_type=jnp.float32)


def after(value, *others):
    return lax.optimization_barrier((value,) + others)[0]


def local_block(x_loc, wq_loc, wk_loc, wv_loc, wo_loc, gq_loc, gk_loc, g_attn, dy_loc):
    batch_size, seq_loc, model_dim = x_loc.shape
    seq_len = seq_loc * N_DEV
    cos_t, sin_t = rope_tables(seq_len)
    gq_row, gk_row = gq_loc[None, :], gk_loc[None, :]
    gq_f, gk_f = gq_row.astype(jnp.float32), gk_row.astype(jnp.float32)

    x_full = lax.all_gather(x_loc, 'tp', axis=1, tiled=True)
    wo_full = lax.all_gather(wo_loc, 'tp', axis=0, tiled=True)
    w_cat = jnp.concatenate([wq_loc, wk_loc, wv_loc], axis=1)
    x_full = after(x_full, w_cat)
    q_raw, k_raw = dot_f32('bsd,de->bse', x_full, wq_loc), dot_f32('bsd,de->bse', x_full, wk_loc)
    v_heads = dot_f32('bsd,de->bse', x_full, wv_loc).astype(jnp.bfloat16)
    part = jnp.stack([jnp.sum(q_raw * q_raw, axis=-1), jnp.sum(k_raw * k_raw, axis=-1)])
    sums = sum_devices(part.reshape(-1, 128)).reshape(2, batch_size, seq_len, 1)
    inv_q, inv_k = lax.rsqrt(sums / model_dim + NORM_EPS)
    heads_out, q_rot, k_rot, lse = attention_fwd(q_raw, k_raw, v_heads, inv_q, inv_k, gq_row, gk_row, cos_t, sin_t)

    o_loc = to_tokens(heads_out).reshape(-1, model_dim)
    attn_loc = dot_f32('te,ed->td', o_loc, wo_full)
    x_f = x_loc.reshape(-1, model_dim).astype(jnp.float32)
    dy_f = dy_loc.reshape(-1, model_dim).astype(jnp.float32)
    post_rms = lax.rsqrt(jnp.mean(attn_loc * attn_loc, axis=-1, keepdims=True) + NORM_EPS)
    normed = attn_loc * post_rms
    ga_f = g_attn.astype(jnp.float32)
    y_loc = (x_f + normed * ga_f).astype(jnp.bfloat16)

    ga_part = jnp.sum(dy_f * normed, axis=0)
    g_normed = dy_f * ga_f
    d_attn = (post_rms * (g_normed - normed * jnp.mean(g_normed * normed, axis=-1, keepdims=True))).astype(jnp.bfloat16)
    d_o_loc = dot_f32('td,ed->te', d_attn, wo_full).astype(jnp.bfloat16)
    d_heads = to_heads(d_o_loc.reshape(batch_size, seq_loc, model_dim))
    d_attn_full = lax.all_gather(d_attn.reshape(batch_size, seq_loc, model_dim), 'tp', axis=1, tiled=True)

    dq_hat, dk_hat, d_value = attention_bwd(q_rot, k_rot, v_heads, d_heads, lse, cos_t, sin_t)
    q_unit, k_unit = q_raw * inv_q, k_raw * inv_k
    dq_unit, dk_unit = dq_hat * gq_f, dk_hat * gk_f
    grad_gq = jnp.sum(dq_hat * q_unit, axis=(0, 1))
    grad_gk = jnp.sum(dk_hat * k_unit, axis=(0, 1))
    part = jnp.stack([jnp.sum(dq_unit * q_unit, axis=-1), jnp.sum(dk_unit * k_unit, axis=-1)])
    sums = sum_devices(jnp.concatenate([part.reshape(-1, 128), ga_part.reshape(-1, 128)]))
    n_rows = part.size // 128
    unit_dots = (sums[:n_rows] / model_dim).reshape(2, batch_size, seq_len, 1)
    grad_ga = sums[n_rows:].reshape(-1)
    dq_raw = (inv_q * (dq_unit - q_unit * unit_dots[0])).astype(jnp.bfloat16)
    dk_raw = (inv_k * (dk_unit - k_unit * unit_dots[1])).astype(jnp.bfloat16)
    far, near = by_distance(dq_raw, dk_raw, d_value)

    def parts_of(lhs):
        return [dot_f32('te,de->td', lhs, w_cat[lo:hi]) for lo, hi in COLUMN_PARTS]

    sums_0, gate = cross_axis(start_sums(parts_of(far[0]), parts_of(near[0])), 0)
    far_parts = parts_of(after(far[1], *gate))
    near_parts = parts_of(after(near[1], *far_parts))
    sums_1 = start_sums(far_parts, near_parts)
    x_early = after(x_full, *near_parts)
    grad_wq, grad_wk = [dot_f32('bsd,bse->de', x_early, cot).astype(jnp.bfloat16) for cot in (dq_raw, dk_raw)]
    sums_0, gate = cross_axis(sums_after(sums_0, [grad_wq, grad_wk]), 1)
    sums_1, gate = cross_axis(sums_after(sums_1, gate), 0)
    grad_wv = dot_f32('bsd,bse->de', after(x_full, *gate), d_value).astype(jnp.bfloat16)
    grad_wo = dot_f32('bse,bsd->ed', heads_out, after(d_attn_full, grad_wv)).astype(jnp.bfloat16)
    sums_1, gate = cross_axis(sums_after(sums_1, [grad_wo]), 1)
    sums_0, gate = cross_axis(sums_after(sums_0, gate), 2)
    sums_1, gate = cross_axis(sums_after(sums_1, gate), 2)
    dx_sums = (sums_after(sums_0, gate), sums_1)
    grad_x = jnp.stack([finish_sums(dx_sums[b]) + dy_loc[b].astype(jnp.float32) for b in range(batch_size)])
    return (y_loc.reshape(x_loc.shape), grad_x.astype(jnp.bfloat16), grad_wq, grad_wk, grad_wv, grad_wo,
            grad_gq.astype(jnp.bfloat16), grad_gk.astype(jnp.bfloat16), grad_ga.astype(jnp.bfloat16))


def solution(mesh):
    act_spec = P(None, 'tp', None)
    col_spec = P(None, 'tp')
    row_spec = P('tp', None)
    vec_spec = P('tp')
    in_specs = (act_spec, col_spec, col_spec, col_spec, row_spec, vec_spec, vec_spec, P(), act_spec)
    out_specs = (act_spec, act_spec, col_spec, col_spec, col_spec, row_spec, vec_spec, vec_spec, P())

    return jax.shard_map(local_block, mesh=mesh, in_specs=in_specs, out_specs=out_specs, check_vma=False)
```

```python
import functools
import math

import jax
import jax.numpy as jnp
from jax import lax
from jax.experimental import pallas as pl
from jax.experimental.pallas import tpu as pltpu
from jax.sharding import PartitionSpec as P


HEAD_SIZE = 128
ROPE_THETA = 500000.0
NORM_EPS = 1e-6
N_DEV = 16
Q_BLOCK = 256
LOG2E = math.log2(math.e)
ATTN_SCALE = HEAD_SIZE ** -0.5
NT = (((1,), (1,)), ((), ()))
NN = (((1,), (0,)), ((), ()))


def rope_tables(seq_len):
    half_dim = HEAD_SIZE // 2
    inv_freq = 1.0 / (ROPE_THETA ** (jnp.arange(half_dim, dtype=jnp.float32) / half_dim))
    angles = jnp.arange(seq_len, dtype=jnp.float32)[:, None] * inv_freq[None, :]
    cos_t, sin_t = jnp.cos(angles), jnp.sin(angles)
    return jnp.concatenate([cos_t, cos_t], axis=-1), jnp.concatenate([-sin_t, sin_t], axis=-1)


def vmem_spec():
    return pl.BlockSpec(memory_space=pltpu.VMEM)


def sum_kernel(part_ref, out_ref, slots, own_sum, send_sems, recv_sems):
    me = lax.axis_index('tp')
    copies = []
    for step in range(1, N_DEV):
        peer = lax.rem(me + step, N_DEV)
        copy = pltpu.make_async_remote_copy(
            src_ref=part_ref.at[peer], dst_ref=slots.at[step], send_sem=send_sems.at[0, step],
            recv_sem=recv_sems.at[0, step], device_id=(peer,), device_id_type=pl.DeviceIdType.MESH)
        copy.start()
        copies.append(copy)
    slots[0] = part_ref[me]
    for copy in copies:
        copy.wait()
    total = slots[0]
    for step in range(1, N_DEV):
        total = total + slots[step]
    own_sum[...] = total
    out_ref[me] = total
    copies = []
    for step in range(1, N_DEV):
        peer = lax.rem(me + step, N_DEV)
        copy = pltpu.make_async_remote_copy(
            src_ref=own_sum, dst_ref=out_ref.at[me], send_sem=send_sems.at[1, step],
            recv_sem=recv_sems.at[1, step], device_id=(peer,), device_id_type=pl.DeviceIdType.MESH)
        copy.start()
        copies.append(copy)
    for copy in copies:
        copy.wait()


def sum_devices(part):
    part = part.reshape(N_DEV, -1, 128)
    return pl.pallas_call(
        sum_kernel,
        out_shape=jax.ShapeDtypeStruct(part.shape, jnp.float32),
        in_specs=[vmem_spec()],
        out_specs=vmem_spec(),
        scratch_shapes=[pltpu.VMEM(part.shape, jnp.float32), pltpu.VMEM(part.shape[1:], jnp.float32),
                        pltpu.SemaphoreType.DMA((2, N_DEV)), pltpu.SemaphoreType.DMA((2, N_DEV))],
        compiler_params=pltpu.CompilerParams(has_side_effects=True),
        cost_estimate=pl.CostEstimate(flops=int(1e9), bytes_accessed=int(1e6), transcendentals=0),
        name='sum_devices',
    )(part).reshape(-1, 128)


def to_tokens_kernel(tok, cols, in_ref, out_ref, send_sems, recv_sems):
    me = lax.axis_index('tp')
    copies = []
    my_cols = pl.ds(pl.multiple_of(me * cols, cols), cols)
    for step in range(1, N_DEV):
        peer = lax.rem(me + step, N_DEV)
        copy = pltpu.make_async_remote_copy(
            src_ref=in_ref.at[:, pl.ds(pl.multiple_of(peer * tok, tok), tok), :], dst_ref=out_ref.at[:, :, my_cols],
            send_sem=send_sems.at[step], recv_sem=recv_sems.at[step],
            device_id=(peer,), device_id_type=pl.DeviceIdType.MESH)
        copy.start()
        copies.append(copy)
    out_ref[:, :, my_cols] = in_ref[:, pl.ds(pl.multiple_of(me * tok, tok), tok), :]
    for copy in copies:
        copy.wait()


def to_heads_kernel(tok, cols, in_ref, out_ref, send_sems, recv_sems):
    me = lax.axis_index('tp')
    my_rows = pl.ds(pl.multiple_of(me * tok, tok), tok)
    copies = []
    for step in range(1, N_DEV):
        peer = lax.rem(me + step, N_DEV)
        copy = pltpu.make_async_remote_copy(
            src_ref=in_ref.at[:, :, pl.ds(pl.multiple_of(peer * cols, cols), cols)], dst_ref=out_ref.at[:, my_rows, :],
            send_sem=send_sems.at[step], recv_sem=recv_sems.at[step],
            device_id=(peer,), device_id_type=pl.DeviceIdType.MESH)
        copy.start()
        copies.append(copy)
    out_ref[:, my_rows, :] = in_ref[:, :, pl.ds(pl.multiple_of(me * cols, cols), cols)]
    for copy in copies:
        copy.wait()


def exchange(kernel, arr, tok, cols, out_shape):
    return pl.pallas_call(
        functools.partial(kernel, tok, cols),
        out_shape=jax.ShapeDtypeStruct(out_shape, jnp.bfloat16),
        in_specs=[vmem_spec()],
        out_specs=vmem_spec(),
        scratch_shapes=[pltpu.SemaphoreType.DMA((N_DEV,)), pltpu.SemaphoreType.DMA((N_DEV,))],
        compiler_params=pltpu.CompilerParams(has_side_effects=True),
        cost_estimate=pl.CostEstimate(flops=int(1e10), bytes_accessed=int(8e6), transcendentals=0),
    )(arr)


def to_tokens(arr):
    batch_size, seq_len, cols = arr.shape
    tok = seq_len // N_DEV
    return exchange(to_tokens_kernel, arr, tok, cols, (batch_size, tok, cols * N_DEV))


def to_heads(arr):
    batch_size, tok, width = arr.shape
    cols = width // N_DEV
    return exchange(to_heads_kernel, arr, tok, cols, (batch_size, tok * N_DEV, cols))


def causal_tile(scores, first_key_row):
    diag = scores[first_key_row:, :]
    key_pos = lax.broadcasted_iota(jnp.int32, diag.shape, 0)
    query_pos = lax.broadcasted_iota(jnp.int32, diag.shape, 1)
    diag = jnp.where(key_pos <= query_pos, diag, -1e30)
    if first_key_row == 0:
        return diag
    return jnp.concatenate([scores[:first_key_row, :], diag], axis=0)


def fwd_kernel(q_ref, k_ref, v_ref, iq_ref, ik_ref, gq_ref, gk_ref, cos_ref, sin_ref,
               o_ref, qr_ref, kr_ref, lse_ref, vt_ref):
    seq_len = q_ref.shape[0]
    cos_t, sin_t = cos_ref[...], sin_ref[...]
    for src, inv, gain, dst in ((q_ref, iq_ref, gq_ref, qr_ref), (k_ref, ik_ref, gk_ref, kr_ref)):
        hat = src[...] * inv[...] * gain[...].astype(jnp.float32)
        dst[...] = (hat * cos_t + pltpu.roll(hat, HEAD_SIZE // 2, 1) * sin_t).astype(jnp.bfloat16)
    vt_ref[...] = v_ref[...].astype(jnp.float32).T.astype(jnp.bfloat16)
    for first in range(0, seq_len, Q_BLOCK):
        ext = first + Q_BLOCK
        scores = lax.dot_general(kr_ref[:ext, :], qr_ref[first:ext, :], NT,
                                 preferred_element_type=jnp.float32) * (ATTN_SCALE * LOG2E)
        scores = causal_tile(scores, first)
        top = jnp.max(scores, axis=0, keepdims=True)
        expd = jnp.exp2(scores - top)
        total = jnp.sum(expd, axis=0, keepdims=True)
        probs = (expd * (1.0 / total)).astype(jnp.bfloat16)
        out_t = lax.dot_general(vt_ref[:, :ext], probs, NN, preferred_element_type=jnp.float32)
        o_ref[first:ext, :] = out_t.T.astype(jnp.bfloat16)
        lse_ref[:, first:ext] = top + jnp.log2(total)


def attention_fwd(q_raw, k_raw, v_heads, inv_q, inv_k, gq, gk, cos_t, sin_t):
    batch_size, seq_len, cols = q_raw.shape
    heads = cols // HEAD_SIZE
    head_spec = pl.BlockSpec((None, seq_len, HEAD_SIZE), lambda b, h: (b, 0, h))
    col_spec = pl.BlockSpec((None, seq_len, 1), lambda b, h: (b, 0, 0))
    gain_spec = pl.BlockSpec((1, HEAD_SIZE), lambda b, h: (0, h))
    table_spec = pl.BlockSpec((seq_len, HEAD_SIZE), lambda b, h: (0, 0))
    lse_spec = pl.BlockSpec((None, None, 1, seq_len), lambda b, h: (b, h, 0, 0))
    return pl.pallas_call(
        fwd_kernel,
        grid=(batch_size, heads),
        in_specs=[head_spec, head_spec, head_spec, col_spec, col_spec, gain_spec, gain_spec, table_spec, table_spec],
        out_specs=[head_spec, head_spec, head_spec, lse_spec],
        out_shape=[jax.ShapeDtypeStruct((batch_size, seq_len, cols), jnp.bfloat16)] * 3
        + [jax.ShapeDtypeStruct((batch_size, heads, 1, seq_len), jnp.float32)],
        scratch_shapes=[pltpu.VMEM((HEAD_SIZE, seq_len), jnp.bfloat16)],
        compiler_params=pltpu.CompilerParams(dimension_semantics=('arbitrary', 'arbitrary'), vmem_limit_bytes=56 * 2 ** 20),
        cost_estimate=pl.CostEstimate(flops=int(8e9), bytes_accessed=int(1e7), transcendentals=int(5e6)),
        name='attention_fwd',
    )(q_raw, k_raw, v_heads, inv_q, inv_k, gq, gk, cos_t, sin_t)


def bwd_kernel(q_ref, k_ref, v_ref, do_ref, lse_ref, cos_ref, sin_ref, dq_ref, dk_ref, dv_ref, kt_ref, dva_ref):
    seq_len = q_ref.shape[0]
    kt_ref[...] = k_ref[...].astype(jnp.float32).T.astype(jnp.bfloat16)
    dk_ref[...] = jnp.zeros_like(dk_ref)
    dva_ref[...] = jnp.zeros_like(dva_ref)
    for first in range(0, seq_len, Q_BLOCK):
        ext = first + Q_BLOCK
        q_blk, do_blk = q_ref[first:ext, :], do_ref[first:ext, :]
        scores = lax.dot_general(k_ref[:ext, :], q_blk, NT,
                                 preferred_element_type=jnp.float32) * (ATTN_SCALE * LOG2E)
        scores = causal_tile(scores, first)
        probs = jnp.exp2(scores - lse_ref[:, first:ext])
        d_probs = lax.dot_general(v_ref[:ext, :], do_blk, NT, preferred_element_type=jnp.float32)
        delta = jnp.sum(probs * d_probs, axis=0, keepdims=True)
        d_scores = (probs * (d_probs - delta) * ATTN_SCALE).astype(jnp.bfloat16)
        dva_ref[:ext, :] += lax.dot_general(probs.astype(jnp.bfloat16), do_blk, NN, preferred_element_type=jnp.float32)
        dk_ref[:ext, :] += lax.dot_general(d_scores, q_blk, NN, preferred_element_type=jnp.float32)
        dq_t = lax.dot_general(kt_ref[:, :ext], d_scores, NN, preferred_element_type=jnp.float32)
        dq = dq_t.T
        dq_ref[first:ext, :] = dq * cos_ref[first:ext, :] - pltpu.roll(dq, HEAD_SIZE // 2, 1) * sin_ref[first:ext, :]
    dk = dk_ref[...]
    dk_ref[...] = dk * cos_ref[...] - pltpu.roll(dk, HEAD_SIZE // 2, 1) * sin_ref[...]
    dv_ref[...] = dva_ref[...].astype(jnp.bfloat16)


def attention_bwd(q_rot, k_rot, v_heads, d_heads, lse, cos_t, sin_t):
    batch_size, seq_len, cols = q_rot.shape
    heads = cols // HEAD_SIZE
    head_spec = pl.BlockSpec((None, seq_len, HEAD_SIZE), lambda b, h: (b, 0, h))
    table_spec = pl.BlockSpec((seq_len, HEAD_SIZE), lambda b, h: (0, 0))
    lse_spec = pl.BlockSpec((None, None, 1, seq_len), lambda b, h: (b, h, 0, 0))
    return pl.pallas_call(
        bwd_kernel,
        grid=(batch_size, heads),
        in_specs=[head_spec, head_spec, head_spec, head_spec, lse_spec, table_spec, table_spec],
        out_specs=[head_spec, head_spec, head_spec],
        out_shape=[jax.ShapeDtypeStruct((batch_size, seq_len, cols), jnp.float32)] * 2
        + [jax.ShapeDtypeStruct((batch_size, seq_len, cols), jnp.bfloat16)],
        scratch_shapes=[pltpu.VMEM((HEAD_SIZE, seq_len), jnp.bfloat16), pltpu.VMEM((seq_len, HEAD_SIZE), jnp.float32)],
        compiler_params=pltpu.CompilerParams(dimension_semantics=('arbitrary', 'arbitrary'), vmem_limit_bytes=56 * 2 ** 20),
        cost_estimate=pl.CostEstimate(flops=int(2e10), bytes_accessed=int(1e7), transcendentals=int(5e6)),
        name='attention_bwd',
    )(q_rot, k_rot, v_heads, d_heads, lse, cos_t, sin_t)


COLUMN_PARTS = ((0, 1280), (1280, 2688), (2688, 4096))
AXIS_ORDERS = ((0, 1, 2), (1, 2, 0), (2, 0, 1))


def by_distance_kernel(tok, cols, dq_ref, dk_ref, dv_ref, *out_refs):
    me = lax.axis_index('tp')
    for b in range(2):
        for side in range(2):
            for chip in range(N_DEV // 2):
                owner = (2 * chip + 1 - side) ^ me
                rows = pl.ds(pl.multiple_of(owner * tok, tok), tok)
                for i, ref in enumerate((dq_ref, dk_ref, dv_ref)):
                    out_refs[2 * b + side][chip * tok:(chip + 1) * tok, i * cols:(i + 1) * cols] = ref[b, rows, :]


def by_distance(dq, dk, dv):
    _, seq_len, cols = dq.shape
    far_0, near_0, far_1, near_1 = pl.pallas_call(
        functools.partial(by_distance_kernel, seq_len // N_DEV, cols),
        in_specs=[vmem_spec()] * 3,
        out_specs=[vmem_spec()] * 4,
        out_shape=[jax.ShapeDtypeStruct((seq_len // 2, 3 * cols), jnp.bfloat16)] * 4,
        compiler_params=pltpu.CompilerParams(vmem_limit_bytes=40 * 2 ** 20),
        cost_estimate=pl.CostEstimate(flops=int(1e9), bytes_accessed=int(12e6), transcendentals=0),
        name='by_distance',
    )(dq, dk, dv)
    return (far_0, far_1), (near_0, near_1)


def flip(value, bit):
    return lax.ppermute(value, 'tp', [(i, i ^ bit) for i in range(N_DEV)])


def start_sums(far, near):
    shape = (2, 2, 2, near[0].shape[0] // 8)
    return [[n.reshape(shape + n.shape[1:]), flip(f, 1).reshape(shape + n.shape[1:])] for f, n in zip(far, near)]


def cross_axis(sums, stage):
    aways, kept = [], []
    for pieces, order in zip(sums, AXIS_ORDERS):
        axis = order[stage]
        away = sum(lax.slice_in_dim(p, 1, 2, axis=axis) for p in pieces)
        aways.append(away)
        came = flip(away, 8 >> axis)
        kept.append([sum(lax.slice_in_dim(p, 0, 1, axis=axis) for p in pieces), came])
    return kept, aways


def sums_after(sums, gate):
    flat = lax.optimization_barrier(tuple(p for pieces in sums for p in pieces) + tuple(gate))
    size = len(sums[0])
    return [list(flat[i * size:(i + 1) * size]) for i in range(len(sums))]


def finish_sums(sums):
    return jnp.concatenate([sum(pieces)[0, 0, 0] for pieces in sums], axis=-1)


def dot_f32(spec, lhs, rhs):
    return jnp.einsum(spec, lhs, rhs, preferred_element_type=jnp.float32)


def after(value, *others):
    return lax.optimization_barrier((value,) + others)[0]


def local_block(x_loc, wq_loc, wk_loc, wv_loc, wo_loc, gq_loc, gk_loc, g_attn, dy_loc):
    batch_size, seq_loc, model_dim = x_loc.shape
    seq_len = seq_loc * N_DEV
    cos_t, sin_t = rope_tables(seq_len)
    gq_row, gk_row = gq_loc[None, :], gk_loc[None, :]
    gq_f, gk_f = gq_row.astype(jnp.float32), gk_row.astype(jnp.float32)

    x_full = lax.all_gather(x_loc, 'tp', axis=1, tiled=True)
    wo_full = lax.all_gather(wo_loc, 'tp', axis=0, tiled=True)
    w_cat = jnp.concatenate([wq_loc, wk_loc, wv_loc], axis=1)
    x_full = after(x_full, w_cat)
    q_raw, k_raw = dot_f32('bsd,de->bse', x_full, wq_loc), dot_f32('bsd,de->bse', x_full, wk_loc)
    v_heads = dot_f32('bsd,de->bse', x_full, wv_loc).astype(jnp.bfloat16)
    q_raw, k_raw = lax.optimization_barrier((q_raw, k_raw))
    part = jnp.stack([jnp.sum(q_raw * q_raw, axis=-1), jnp.sum(k_raw * k_raw, axis=-1)])
    sums = sum_devices(part.reshape(-1, 128)).reshape(2, batch_size, seq_len, 1)
    inv_q, inv_k = lax.rsqrt(sums / model_dim + NORM_EPS)
    heads_out, q_rot, k_rot, lse = attention_fwd(q_raw, k_raw, v_heads, inv_q, inv_k, gq_row, gk_row, cos_t, sin_t)

    o_loc = to_tokens(heads_out).reshape(-1, model_dim)
    attn_loc = dot_f32('te,ed->td', o_loc, wo_full)
    x_f = x_loc.reshape(-1, model_dim).astype(jnp.float32)
    dy_f = dy_loc.reshape(-1, model_dim).astype(jnp.float32)
    post_rms = lax.rsqrt(jnp.mean(attn_loc * attn_loc, axis=-1, keepdims=True) + NORM_EPS)
    normed = attn_loc * post_rms
    ga_f = g_attn.astype(jnp.float32)
    y_loc = (x_f + normed * ga_f).astype(jnp.bfloat16)

    ga_part = jnp.sum(dy_f * normed, axis=0)
    g_normed = dy_f * ga_f
    d_attn = (post_rms * (g_normed - normed * jnp.mean(g_normed * normed, axis=-1, keepdims=True))).astype(jnp.bfloat16)
    d_o_loc = dot_f32('td,ed->te', d_attn, wo_full).astype(jnp.bfloat16)
    d_heads = to_heads(d_o_loc.reshape(batch_size, seq_loc, model_dim))
    d_attn_full = lax.all_gather(after(d_attn.reshape(batch_size, seq_loc, model_dim), d_heads), 'tp', axis=1, tiled=True)

    dq_hat, dk_hat, d_value = attention_bwd(q_rot, k_rot, v_heads, d_heads, lse, cos_t, sin_t)
    q_unit, k_unit = q_raw * inv_q, k_raw * inv_k
    dq_unit, dk_unit = dq_hat * gq_f, dk_hat * gk_f
    grad_gq = jnp.sum(dq_hat * q_unit, axis=(0, 1))
    grad_gk = jnp.sum(dk_hat * k_unit, axis=(0, 1))
    part = jnp.stack([jnp.sum(dq_unit * q_unit, axis=-1), jnp.sum(dk_unit * k_unit, axis=-1)])
    sums = sum_devices(jnp.concatenate([part.reshape(-1, 128), ga_part.reshape(-1, 128)]))
    n_rows = part.size // 128
    unit_dots = (sums[:n_rows] / model_dim).reshape(2, batch_size, seq_len, 1)
    grad_ga = sums[n_rows:].reshape(-1)
    dq_raw = (inv_q * (dq_unit - q_unit * unit_dots[0])).astype(jnp.bfloat16)
    dk_raw = (inv_k * (dk_unit - k_unit * unit_dots[1])).astype(jnp.bfloat16)
    far, near = by_distance(dq_raw, dk_raw, d_value)

    def parts_of(lhs):
        return [dot_f32('te,de->td', lhs, w_cat[lo:hi]) for lo, hi in COLUMN_PARTS]

    sums_0, gate = cross_axis(start_sums(parts_of(far[0]), parts_of(near[0])), 0)
    far_parts = parts_of(after(far[1], *gate))
    near_parts = parts_of(after(near[1], *far_parts))
    sums_1, gate = cross_axis(start_sums(far_parts, near_parts), 0)
    x_early = after(x_full, *gate)
    grad_wq, grad_wk = [dot_f32('bsd,bse->de', x_early, cot).astype(jnp.bfloat16) for cot in (dq_raw, dk_raw)]
    sums_0, gate = cross_axis(sums_after(sums_0, [grad_wq, grad_wk]), 1)
    grad_wv = dot_f32('bsd,bse->de', after(x_full, *gate), d_value).astype(jnp.bfloat16)
    grad_wo = dot_f32('bse,bsd->ed', heads_out, after(d_attn_full, grad_wv)).astype(jnp.bfloat16)
    sums_1, gate = cross_axis(sums_after(sums_1, [grad_wo]), 1)
    sums_0, gate = cross_axis(sums_after(sums_0, gate), 2)
    sums_1, gate = cross_axis(sums_after(sums_1, gate), 2)
    dx_sums = (sums_after(sums_0, gate), sums_1)
    grad_x = jnp.stack([finish_sums(dx_sums[b]) + dy_loc[b].astype(jnp.float32) for b in range(batch_size)])
    return (y_loc.reshape(x_loc.shape), grad_x.astype(jnp.bfloat16), grad_wq, grad_wk, grad_wv, grad_wo,
            grad_gq.astype(jnp.bfloat16), grad_gk.astype(jnp.bfloat16), grad_ga.astype(jnp.bfloat16))


def solution(mesh):
    act_spec = P(None, 'tp', None)
    col_spec = P(None, 'tp')
    row_spec = P('tp', None)
    vec_spec = P('tp')
    in_specs = (act_spec, col_spec, col_spec, col_spec, row_spec, vec_spec, vec_spec, P(), act_spec)
    out_specs = (act_spec, act_spec, col_spec, col_spec, col_spec, row_spec, vec_spec, vec_spec, P())

    return jax.shard_map(local_block, mesh=mesh, in_specs=in_specs, out_specs=out_specs, check_vma=False)
```
